8 devices in a mesh: parts: 1 (over z), col: 2 (over y), row: 2 (over x), sub: 2 (over core).
Axes of the slice: x: 2, y: 2, z: 1, core: 2. Of those that a mesh axis runs over, the one named last changes fastest.
Arguments:
- edge_dist: float32 [16, 128, 2048], P(('parts', 'row', 'sub'), None, 'col')
Outputs:
- output: float32 [16, 128, 2048], P(('parts', 'row', 'sub'), None, 'col')
All inputs are finite; a program needn't handle non-finite values.
Results may differ from the reference program's by a relative error of at most 0.001.
Values sent between devices are 32-bit elements.
A program may use at most 1 GiB of HBM per device.

```python
import jax
import jax.numpy as jnp
from jax import lax

VERTICES = 2048
BLOCK = 128
ROW_DEVS = 4
COL_DEVS = 2
CHORDS = 2

ROUNDS = VERTICES // BLOCK
NO_EDGE = 2 ** 16


def to_stored(full_dist):
    by_rows = full_dist.reshape(ROUNDS // ROW_DEVS, ROW_DEVS, BLOCK, VERTICES).transpose(1, 0, 2, 3)
    by_rows = by_rows.reshape(ROUNDS, BLOCK, ROUNDS // COL_DEVS, COL_DEVS, BLOCK).transpose(0, 1, 3, 2, 4)
    return by_rows.reshape(ROUNDS, BLOCK, VERTICES)


def from_stored(stored):
    by_cols = stored.reshape(ROUNDS, BLOCK, COL_DEVS, ROUNDS // COL_DEVS, BLOCK).transpose(0, 1, 3, 2, 4)
    by_cols = by_cols.reshape(ROW_DEVS, ROUNDS // ROW_DEVS, BLOCK, VERTICES).transpose(1, 0, 2, 3)
    return by_cols.reshape(VERTICES, VERTICES)


def setup_inputs(seed: int = 0, part: int = 0) -> dict:
    base_key = jax.random.fold_in(jax.random.key(seed), part)
    key_cycle, key_dst, key_wt = jax.random.split(base_key, 3)
    vertex_ids = jnp.arange(VERTICES)
    cycle_wt = jax.random.randint(key_cycle, (VERTICES,), 8, 17).astype(jnp.float32) / 8.0
    chord_dst = jax.random.randint(key_dst, (VERTICES, CHORDS), 0, VERTICES)
    chord_wt = jax.random.randint(key_wt, (VERTICES, CHORDS), 1, 17).astype(jnp.float32) / 8.0
    full_dist = jnp.full((VERTICES, VERTICES), NO_EDGE, dtype=jnp.float32)
    full_dist = full_dist.at[vertex_ids, (vertex_ids + 1) % VERTICES].min(cycle_wt)
    full_dist = full_dist.at[vertex_ids[:, None], chord_dst].min(chord_wt)
    full_dist = full_dist.at[vertex_ids, vertex_ids].set(0.0)
    return {'edge_dist': to_stored(full_dist)}


def close_block(block_in):
    def pivot_step(pivot_idx, current):
        col_vec = lax.dynamic_slice_in_dim(current, pivot_idx, 1, axis=1)
        row_vec = lax.dynamic_slice_in_dim(current, pivot_idx, 1, axis=0)
        return jnp.minimum(current, col_vec + row_vec)
    return lax.fori_loop(0, block_in.shape[0], pivot_step, block_in)


def min_plus(left_mat, right_mat):
    num_rows = left_mat.shape[0]
    row_groups = left_mat.reshape(num_rows // 8, 8, left_mat.shape[1])
    result = lax.map(lambda row_group: jnp.min(row_group[:, :, None] + right_mat[None, :, :], axis=1), row_groups)
    return result.reshape(num_rows, right_mat.shape[1])


def reference(edge_dist):
    def one_round(current, round_idx):
        offset = round_idx * BLOCK
        diag_blk = close_block(lax.dynamic_slice(current, (offset, offset), (BLOCK, BLOCK)))
        row_pan = min_plus(diag_blk, lax.dynamic_slice_in_dim(current, offset, BLOCK, axis=0))
        col_pan = min_plus(lax.dynamic_slice_in_dim(current, offset, BLOCK, axis=1), diag_blk)
        return jnp.minimum(current, min_plus(col_pan, row_pan)), None
    full_dist = lax.scan(one_round, from_stored(edge_dist), jnp.arange(ROUNDS))[0]
    return to_stored(full_dist)
```

```python
import functools

import jax
import jax.numpy as jnp
from jax import lax
from jax.experimental import pallas as pl
from jax.experimental.pallas import tpu as pltpu
from jax.sharding import PartitionSpec as P

MESH = pl.DeviceIdType.MESH
CHUNK = 16
GROUP = 8


def close_block(src, dst, spread):
    size = src.shape[0]
    tiles_n = size // GROUP
    tile_of = lambda x: jnp.broadcast_to(x, (GROUP, size))
    tiles = [src[GROUP * i:GROUP * (i + 1), :] for i in range(tiles_n)]
    for g in range(tiles_n):
        column = lambda i, b: tile_of(tiles[i][:, GROUP * g + b:GROUP * g + b + 1])
        own = [column(g, b) for b in range(GROUP)]
        for b in range(GROUP):
            spread[b] = own[b]
        spread[GROUP] = tiles[g]
        rows = [tile_of(spread[GROUP, b:b + 1, :]) for b in range(GROUP)]
        entry = [[tile_of(spread[b, a:a + 1, :]) for b in range(GROUP)] for a in range(GROUP)]
        for m in range(GROUP):
            for a in range(GROUP):
                if a == m:
                    continue
                rows[a] = jnp.minimum(rows[a], entry[a][m] + rows[m])
                for b in range(m + 1, GROUP):
                    if a != b:
                        entry[a][b] = jnp.minimum(entry[a][b], entry[a][m] + entry[m][b])
        for i in [(g + 1 + n) % tiles_n for n in range(tiles_n)]:
            cols = own if i == g else [column(i, b) for b in range(GROUP)]
            for b in range(GROUP):
                tiles[i] = jnp.minimum(tiles[i], cols[b] + rows[b])
    for i in range(tiles_n):
        dst[GROUP * i:GROUP * (i + 1), :] = tiles[i]


def min_plus_rows(left, right, init, out):
    left_rows = left[...]
    acc = init[...]
    for l in range(left.shape[1]):
        acc = jnp.minimum(acc, left_rows[:, l:l + 1][None] + right[:, l:l + 1, :])
    out[...] = acc


def kernel(rounds, row_devs, sub_devs, x_hbm, o_hbm, cur, row_pan, col_pan, diag, spread,
           in_sem, out_sem, row_send, row_recv, relay_send, col_send, col_recv, diag_send, diag_recv):
    col_blks, row_blks, blk, _ = cur.shape
    chunks = blk // CHUNK
    half = blk // sub_devs
    col_devs = rounds // col_blks
    x = lax.axis_index('row')
    sub = lax.axis_index('sub')
    c = lax.axis_index('col')
    r = x * sub_devs + sub
    other_x, other_sub, other_c = 1 - x, 1 - sub, 1 - c
    peers = [{'row': x, 'sub': other_sub}, {'row': other_x, 'sub': sub}, {'row': other_x, 'sub': other_sub},
             {'col': other_c}]

    loads = [pltpu.make_async_copy(x_hbm.at[:, :, j * blk:(j + 1) * blk], cur.at[j], in_sem.at[j])
             for j in range(col_blks)]
    for load in loads:
        load.start()
    barrier = pltpu.get_barrier_semaphore()
    for peer in peers:
        pl.semaphore_signal(barrier, inc=1, device_id=peer, device_id_type=MESH)
    pl.semaphore_wait(barrier, len(peers))
    for load in loads:
        load.wait()

    def to_sibling(n, lo, count, recv):
        part = row_pan.at[n, :, pl.ds(lo, count), :]
        return pltpu.make_async_remote_copy(part, part, row_send.at[n, 0], row_recv.at[n, recv],
                                            device_id={'sub': other_sub}, device_id_type=MESH)

    def to_chip(n, lo, count, sub_to):
        part = row_pan.at[n, :, pl.ds(lo, count), :]
        return pltpu.make_async_remote_copy(part, part, row_send.at[n, 1], row_recv.at[n, 0],
                                            device_id={'row': other_x, 'sub': sub_to}, device_id_type=MESH)

    def relay(n, lo):
        part = row_pan.at[n, :, pl.ds(lo, half), :]
        return pltpu.make_async_remote_copy(part, part, relay_send.at[n], row_recv.at[n, 1],
                                            device_id={'sub': other_sub}, device_id_type=MESH)

    def col_copy(n, b):
        part = col_pan.at[n, b]
        return pltpu.make_async_remote_copy(part, part, col_send.at[n], col_recv.at[n, b],
                                            device_id={'col': other_c}, device_id_type=MESH)

    def diag_copy(n):
        return pltpu.make_async_remote_copy(diag.at[n], diag.at[n], diag_send.at[n], diag_recv.at[n],
                                            device_id={'col': other_c}, device_id_type=MESH)

    def out_copies(b):
        return [pltpu.make_async_copy(cur.at[j, b], o_hbm.at[b, :, j * blk:(j + 1) * blk],
                                      out_sem.at[b, j])
                for j in range(col_blks)]

    def one_round(step, carry):
        k = step - 1
        nxt = step
        has_main = step > 0
        has_next = step < rounds
        own_k = (step + row_devs - 1) % row_devs
        own_n = step % row_devs
        is_owner = has_main & (r == own_k)
        is_next = has_next & (r == own_n)
        col_owner = has_main & (c == (step + col_devs - 1) % col_devs)
        col_next = has_next & (c == step % col_devs)
        first = ((step - r + 2 + row_devs) // row_devs + row_blks - 1) % row_blks
        k_c = lax.max(k, 0)
        n_c = lax.min(nxt, rounds - 1)
        q = n_c // col_devs
        far_k = x != own_k // sub_devs
        far_n = has_next & (x != own_n // sub_devs)
        my_lo = sub * half
        other_lo = other_sub * half

        @pl.when(has_main & far_k)
        def _():
            pltpu.make_async_remote_copy(
                row_pan.at[k_c, :, pl.ds(other_lo, half), :], row_pan.at[k_c, :, pl.ds(other_lo, half), :],
                relay_send.at[k_c], row_recv.at[k_c, 1], device_id={'sub': other_sub}, device_id_type=MESH).wait_recv()

        @pl.when(has_main & jnp.logical_not(far_k) & jnp.logical_not(is_owner))
        def _():
            to_sibling(k_c, 0, blk, 0).wait_recv()

        def one_chunk(t, carry):
            i = t // chunks
            ch = t % chunks
            b = (first + i) % row_blks
            lo = pl.multiple_of(ch * CHUNK, CHUNK)
            active = has_main & jnp.logical_not(is_owner & (i == 0))

            @pl.when(active & (ch == 0) & jnp.logical_not(col_owner))
            def _():
                col_copy(k_c, b).wait_recv()

            @pl.when(active)
            def _():
                mine = cur.at[:, b, pl.ds(lo, CHUNK), :]
                min_plus_rows(col_pan.at[k_c, b, pl.ds(lo, CHUNK), :], row_pan.at[k_c], mine, mine)

            @pl.when((ch == chunks - 1) & col_next)
            def _():
                col_pan[n_c, b] = cur[q, b]

                @pl.when(jnp.logical_not(is_next & (i == 0)))
                def _():
                    col_copy(n_c, b).start()

            @pl.when((ch == chunks - 1) & (step == rounds))
            def _():
                for copy in out_copies(b):
                    copy.start()

            @pl.when((t == chunks - 1) & is_next & col_next)
            def _():
                close_block(col_pan.at[n_c, b], diag.at[n_c], spread)
                diag_copy(n_c).start()

            @pl.when((t == 2 * chunks - 1) & is_next)
            def _():
                @pl.when(jnp.logical_not(col_next))
                def _():
                    diag_copy(n_c).wait_recv()

                def panel_chunk(h, carry):
                    at = pl.multiple_of(h * CHUNK, CHUNK)
                    min_plus_rows(diag.at[n_c, pl.ds(at, CHUNK), :], cur.at[:, first],
                                  cur.at[:, first, pl.ds(at, CHUNK), :], row_pan.at[n_c, :, pl.ds(at, CHUNK), :])
                    to_sibling(n_c, at, CHUNK, 0).start()
                    to_chip(n_c, at, CHUNK, at // half).start()
                    return carry
                lax.fori_loop(0, chunks, panel_chunk, 0)
                cur[:, first] = row_pan[n_c]

            @pl.when((t == (row_blks - 1) * chunks + chunks // 2 - 1) & far_n)
            def _():
                to_chip(n_c, my_lo, half, sub).wait_recv()
                relay(n_c, my_lo).start()
            return carry

        lax.fori_loop(0, row_blks * chunks, one_chunk, 0)

        @pl.when(is_owner)
        def _():
            to_sibling(k_c, 0, blk, 0).wait_send()
            to_chip(k_c, 0, blk, 0).wait_send()

        @pl.when(is_owner & col_owner)
        def _():
            diag_copy(k_c).wait_send()

        @pl.when(has_main & far_k)
        def _():
            relay(k_c, my_lo).wait_send()

        @pl.when(col_owner)
        def _():
            for i in range(row_blks):
                @pl.when(jnp.logical_not(is_owner & (first == i)))
                def _():
                    col_copy(k_c, i).wait_send()
        return carry

    lax.fori_loop(0, rounds + 1, one_round, 0)
    for b in range(row_blks):
        for copy in out_copies(b):
            copy.wait()


def solution(mesh):
    sub_devs = mesh.shape['sub']
    row_devs = mesh.shape['row'] * sub_devs
    col_devs = mesh.shape['col']
    dist_spec = P(('parts', 'row', 'sub'), None, 'col')

    def local_run(local_dist):
        row_blks, blk, cols_width = local_dist.shape
        col_blks = cols_width // blk
        rounds = row_blks * row_devs
        dma = pltpu.SemaphoreType.DMA
        return pl.pallas_call(
            functools.partial(kernel, rounds, row_devs, sub_devs),
            out_shape=jax.ShapeDtypeStruct(local_dist.shape, local_dist.dtype),
            in_specs=[pl.BlockSpec(memory_space=pl.ANY)],
            out_specs=pl.BlockSpec(memory_space=pl.ANY),
            scratch_shapes=[
                pltpu.VMEM((col_blks, row_blks, blk, blk), jnp.float32),
                pltpu.VMEM((rounds, col_blks, blk, blk), jnp.float32),
                pltpu.VMEM((rounds, row_blks, blk, blk), jnp.float32),
                pltpu.VMEM((rounds, blk, blk), jnp.float32),
                pltpu.VMEM((GROUP + 1, GROUP, blk), jnp.float32),
                dma((col_blks,)), dma((row_blks, col_blks)),
                dma((rounds, 2)), dma((rounds, 2)), dma((rounds,)),
                dma((rounds,)), dma((rounds, row_blks)),
                dma((rounds,)), dma((rounds,)),
            ],
            compiler_params=pltpu.CompilerParams(
                collective_id=0, has_side_effects=True, vmem_limit_bytes=40 * 1024 * 1024),
            name='apsp',
        )(local_dist)

    return jax.shard_map(local_run, mesh=mesh, in_specs=(dist_spec,), out_specs=dist_spec, check_vma=False)
```

```python
import functools

import jax
import jax.numpy as jnp
from jax import lax
from jax.experimental import pallas as pl
from jax.experimental.pallas import tpu as pltpu
from jax.sharding import PartitionSpec as P

MESH = pl.DeviceIdType.MESH
CHUNK = 16
GROUP = 8
PANEL_AT = 3


def close_block(src, dst, spread):
    size = src.shape[0]
    tiles_n = size // GROUP
    tile_of = lambda x: jnp.broadcast_to(x, (GROUP, size))
    tiles = [src[GROUP * i:GROUP * (i + 1), :] for i in range(tiles_n)]
    for g in range(tiles_n):
        column = lambda i, b: tile_of(tiles[i][:, GROUP * g + b:GROUP * g + b + 1])
        own = [column(g, b) for b in range(GROUP)]
        for b in range(GROUP):
            spread[b] = own[b]
        spread[GROUP] = tiles[g]
        rows = [tile_of(spread[GROUP, b:b + 1, :]) for b in range(GROUP)]
        entry = [[tile_of(spread[b, a:a + 1, :]) for b in range(GROUP)] for a in range(GROUP)]
        for m in range(GROUP):
            for a in range(GROUP):
                if a == m:
                    continue
                rows[a] = jnp.minimum(rows[a], entry[a][m] + rows[m])
                for b in range(m + 1, GROUP):
                    if a != b:
                        entry[a][b] = jnp.minimum(entry[a][b], entry[a][m] + entry[m][b])
        for i in [(g + 1 + n) % tiles_n for n in range(tiles_n)]:
            cols = own if i == g else [column(i, b) for b in range(GROUP)]
            for b in range(GROUP):
                tiles[i] = jnp.minimum(tiles[i], cols[b] + rows[b])
    for i in range(tiles_n):
        dst[GROUP * i:GROUP * (i + 1), :] = tiles[i]


def min_plus_rows(left, right, init, out):
    left_rows = left[...]
    acc = init[...]
    for l in range(left.shape[1]):
        acc = jnp.minimum(acc, left_rows[:, l:l + 1][None] + right[:, l:l + 1, :])
    out[...] = acc


def kernel(rounds, row_devs, sub_devs, x_hbm, o_hbm, cur, row_pan, col_pan, diag, spread,
           in_sem, out_sem, row_send, row_recv, relay_send, col_send, col_recv, diag_send, diag_recv):
    col_blks, row_blks, blk, _ = cur.shape
    chunks = blk // CHUNK
    half = blk // sub_devs
    col_devs = rounds // col_blks
    x = lax.axis_index('row')
    sub = lax.axis_index('sub')
    c = lax.axis_index('col')
    r = x * sub_devs + sub
    other_x, other_sub, other_c = 1 - x, 1 - sub, 1 - c
    peers = [{'row': x, 'sub': other_sub}, {'row': other_x, 'sub': sub}, {'row': other_x, 'sub': other_sub},
             {'col': other_c}]

    loads = [pltpu.make_async_copy(x_hbm.at[:, :, j * blk:(j + 1) * blk], cur.at[j], in_sem.at[j])
             for j in range(col_blks)]
    for load in loads:
        load.start()
    barrier = pltpu.get_barrier_semaphore()
    for peer in peers:
        pl.semaphore_signal(barrier, inc=1, device_id=peer, device_id_type=MESH)
    pl.semaphore_wait(barrier, len(peers))
    for load in loads:
        load.wait()

    def to_sibling(n, lo, count, recv):
        part = row_pan.at[n, :, pl.ds(lo, count), :]
        return pltpu.make_async_remote_copy(part, part, row_send.at[n, 0], row_recv.at[n, recv],
                                            device_id={'sub': other_sub}, device_id_type=MESH)

    def to_chip(n, lo, count, sub_to):
        part = row_pan.at[n, :, pl.ds(lo, count), :]
        return pltpu.make_async_remote_copy(part, part, row_send.at[n, 1], row_recv.at[n, 0],
                                            device_id={'row': other_x, 'sub': sub_to}, device_id_type=MESH)

    def relay(n, lo):
        part = row_pan.at[n, :, pl.ds(lo, half), :]
        return pltpu.make_async_remote_copy(part, part, relay_send.at[n], row_recv.at[n, 1],
                                            device_id={'sub': other_sub}, device_id_type=MESH)

    def col_copy(n, b):
        part = col_pan.at[n, b]
        return pltpu.make_async_remote_copy(part, part, col_send.at[n], col_recv.at[n, b],
                                            device_id={'col': other_c}, device_id_type=MESH)

    def diag_copy(n):
        return pltpu.make_async_remote_copy(diag.at[n], diag.at[n], diag_send.at[n], diag_recv.at[n],
                                            device_id={'col': other_c}, device_id_type=MESH)

    def out_copies(b):
        return [pltpu.make_async_copy(cur.at[j, b], o_hbm.at[b, :, j * blk:(j + 1) * blk],
                                      out_sem.at[b, j])
                for j in range(col_blks)]

    def one_round(step, carry):
        k = step - 1
        nxt = step
        has_main = step > 0
        has_next = step < rounds
        own_k = (step + row_devs - 1) % row_devs
        own_n = step % row_devs
        is_owner = has_main & (r == own_k)
        is_next = has_next & (r == own_n)
        col_owner = has_main & (c == (step + col_devs - 1) % col_devs)
        col_next = has_next & (c == step % col_devs)
        first = ((step - r + 2 + row_devs) // row_devs + row_blks - 1) % row_blks
        k_c = lax.max(k, 0)
        n_c = lax.min(nxt, rounds - 1)
        q = n_c // col_devs
        far_k = x != own_k // sub_devs
        far_n = has_next & (x != own_n // sub_devs)
        my_lo = sub * half
        other_lo = other_sub * half

        @pl.when(has_main & far_k)
        def _():
            pltpu.make_async_remote_copy(
                row_pan.at[k_c, :, pl.ds(other_lo, half), :], row_pan.at[k_c, :, pl.ds(other_lo, half), :],
                relay_send.at[k_c], row_recv.at[k_c, 1], device_id={'sub': other_sub}, device_id_type=MESH).wait_recv()

        @pl.when(has_main & jnp.logical_not(far_k) & jnp.logical_not(is_owner))
        def _():
            to_sibling(k_c, 0, blk, 0).wait_recv()

        def update(b, lo_chunk, count):
            def one_chunk(h, carry):
                lo = pl.multiple_of((lo_chunk + h) * CHUNK, CHUNK)
                mine = cur.at[:, b, pl.ds(lo, CHUNK), :]
                min_plus_rows(col_pan.at[k_c, b, pl.ds(lo, CHUNK), :], row_pan.at[k_c], mine, mine)
                return carry
            lax.fori_loop(0, count, one_chunk, 0)

        def one_half(t, carry):
            i = t // 2
            h = t % 2
            b = (first + i) % row_blks
            active = has_main & jnp.logical_not(is_owner & (i == 0))

            @pl.when(active & (h == 0) & jnp.logical_not(col_owner))
            def _():
                col_copy(k_c, b).wait_recv()

            update(b, h * (chunks // 2), jnp.where(active, chunks // 2, 0))

            @pl.when((h == 1) & col_next)
            def _():
                col_pan[n_c, b] = cur[q, b]

                @pl.when(jnp.logical_not(is_next & (i == 0)))
                def _():
                    col_copy(n_c, b).start()

            @pl.when((h == 1) & (step == rounds))
            def _():
                for copy in out_copies(b):
                    copy.start()

            @pl.when((t == 1) & is_next & col_next)
            def _():
                close_block(col_pan.at[n_c, b], diag.at[n_c], spread)
                diag_copy(n_c).start()

            @pl.when(is_next & (t == jnp.where(col_next, 1, PANEL_AT)))
            def _():
                @pl.when(jnp.logical_not(col_next))
                def _():
                    diag_copy(n_c).wait_recv()

                def panel_chunk(h, carry):
                    at = pl.multiple_of(h * CHUNK, CHUNK)
                    min_plus_rows(diag.at[n_c, pl.ds(at, CHUNK), :], cur.at[:, first],
                                  cur.at[:, first, pl.ds(at, CHUNK), :], row_pan.at[n_c, :, pl.ds(at, CHUNK), :])
                    to_sibling(n_c, at, CHUNK, 0).start()
                    to_chip(n_c, at, CHUNK, at // half).start()
                    return carry
                lax.fori_loop(0, chunks, panel_chunk, 0)
                cur[:, first] = row_pan[n_c]

            @pl.when((t == 2 * row_blks - 2) & far_n)
            def _():
                to_chip(n_c, my_lo, half, sub).wait_recv()
                relay(n_c, my_lo).start()
            return carry

        lax.fori_loop(0, 2 * row_blks, one_half, 0)

        @pl.when(is_owner)
        def _():
            to_sibling(k_c, 0, blk, 0).wait_send()
            to_chip(k_c, 0, blk, 0).wait_send()

        @pl.when(is_owner & col_owner)
        def _():
            diag_copy(k_c).wait_send()

        @pl.when(has_main & far_k)
        def _():
            relay(k_c, my_lo).wait_send()

        @pl.when(col_owner)
        def _():
            for i in range(row_blks):
                @pl.when(jnp.logical_not(is_owner & (first == i)))
                def _():
                    col_copy(k_c, i).wait_send()
        return carry

    lax.fori_loop(0, rounds + 1, one_round, 0)
    for b in range(row_blks):
        for copy in out_copies(b):
            copy.wait()


def solution(mesh):
    sub_devs = mesh.shape['sub']
    row_devs = mesh.shape['row'] * sub_devs
    col_devs = mesh.shape['col']
    dist_spec = P(('parts', 'row', 'sub'), None, 'col')

    def local_run(local_dist):
        row_blks, blk, cols_width = local_dist.shape
        col_blks = cols_width // blk
        rounds = row_blks * row_devs
        dma = pltpu.SemaphoreType.DMA
        return pl.pallas_call(
            functools.partial(kernel, rounds, row_devs, sub_devs),
            out_shape=jax.ShapeDtypeStruct(local_dist.shape, local_dist.dtype),
            in_specs=[pl.BlockSpec(memory_space=pl.ANY)],
            out_specs=pl.BlockSpec(memory_space=pl.ANY),
            scratch_shapes=[
                pltpu.VMEM((col_blks, row_blks, blk, blk), jnp.float32),
                pltpu.VMEM((rounds, col_blks, blk, blk), jnp.float32),
                pltpu.VMEM((rounds, row_blks, blk, blk), jnp.float32),
                pltpu.VMEM((rounds, blk, blk), jnp.float32),
                pltpu.VMEM((GROUP + 1, GROUP, blk), jnp.float32),
                dma((col_blks,)), dma((row_blks, col_blks)),
                dma((rounds, 2)), dma((rounds, 2)), dma((rounds,)),
                dma((rounds,)), dma((rounds, row_blks)),
                dma((rounds,)), dma((rounds,)),
            ],
            compiler_params=pltpu.CompilerParams(
                collective_id=0, has_side_effects=True, vmem_limit_bytes=40 * 1024 * 1024),
            name='apsp',
        )(local_dist)

    return jax.shard_map(local_run, mesh=mesh, in_specs=(dist_spec,), out_specs=dist_spec, check_vma=False)
```

```python
import functools

import jax
import jax.numpy as jnp
from jax import lax
from jax.experimental import pallas as pl
from jax.experimental.pallas import tpu as pltpu
from jax.sharding import PartitionSpec as P

MESH = pl.DeviceIdType.MESH
CHUNK = 64
PANEL_CHUNK = 16
PART = 16
AHEAD = 104
PAD = 8
RELAY_AT = 6
GROUP = 8
PANEL_AT = 3


def close_block(src, dst, spread):
    size = src.shape[0]
    tiles_n = size // GROUP
    tile_of = lambda x: jnp.broadcast_to(x, (GROUP, size))
    column_of = lambda tile, g, b: tile_of(tile[:, GROUP * g + b:GROUP * g + b + 1])
    tiles = [src[GROUP * i:GROUP * (i + 1), :] for i in range(tiles_n)]
    for g in range(tiles_n):
        own = [column_of(tiles[g], g, b) for b in range(GROUP)]
        for b in range(GROUP):
            spread[b] = own[b]
        spread[GROUP] = tiles[g]
        rows = [tile_of(spread[GROUP, b:b + 1, :]) for b in range(GROUP)]
        entry = [[tile_of(spread[b, a:a + 1, :]) for b in range(GROUP)] for a in range(GROUP)]
        for m in range(GROUP):
            for a in range(GROUP):
                if a == m:
                    continue
                rows[a] = jnp.minimum(rows[a], entry[a][m] + rows[m])
                for b in range(m + 1, GROUP):
                    if a != b:
                        entry[a][b] = jnp.minimum(entry[a][b], entry[a][m] + entry[m][b])
        before = list(tiles)
        following = (g + 1) % tiles_n
        others = [(g + 2 + n) % tiles_n for n in range(tiles_n - 1)]
        for part in ([following], others):
            for b in range(GROUP):
                for i in part:
                    column = own[b] if i == g else column_of(before[i], g, b)
                    tiles[i] = jnp.minimum(tiles[i], column + rows[b])
    for i in range(tiles_n):
        dst[GROUP * i:GROUP * (i + 1), :] = tiles[i]


def min_plus_rows(left, right, init, out):
    parts = left.shape[0] // PART
    left_rows = left[0:PART, :]
    for u in range(parts):
        acc = init[:, u * PART:(u + 1) * PART, :]
        for l in range(left.shape[1]):
            acc = jnp.minimum(acc, left_rows[:, l:l + 1][None] + right[:, l:l + 1, :])
            if l == AHEAD and u + 1 < parts:
                ahead = left[(u + 1) * PART:(u + 2) * PART, :]
                ahead = jnp.minimum(ahead, jnp.maximum(ahead, acc[0]))
        out[:, u * PART:(u + 1) * PART, :] = acc
        left_rows = ahead if u + 1 < parts else None


def kernel(rounds, row_devs, sub_devs, x_hbm, o_hbm, cur, row_pan, col_pan, diag, spread,
           in_sem, out_sem, row_send, row_recv, relay_send, col_send, col_recv, diag_send, diag_recv):
    row_blks, blk = col_pan.shape[1:3]
    col_blks = cur.shape[0]
    chunks = blk // CHUNK
    half = blk // sub_devs
    col_devs = rounds // col_blks
    x = lax.axis_index('row')
    sub = lax.axis_index('sub')
    c = lax.axis_index('col')
    r = x * sub_devs + sub
    other_x, other_sub, other_c = 1 - x, 1 - sub, 1 - c
    peers = [{'row': x, 'sub': other_sub}, {'row': other_x, 'sub': sub}, {'row': other_x, 'sub': other_sub},
             {'col': other_c}]

    def block(b, lo, count):
        return pl.ds(pl.multiple_of(b * blk + lo, PANEL_CHUNK), count)

    loads = [pltpu.make_async_copy(x_hbm.at[b, :, j * blk:(j + 1) * blk], cur.at[j, block(b, 0, blk)], in_sem.at[b, j])
             for b in range(row_blks) for j in range(col_blks)]
    for load in loads:
        load.start()
    barrier = pltpu.get_barrier_semaphore()
    for peer in peers:
        pl.semaphore_signal(barrier, inc=1, device_id=peer, device_id_type=MESH)
    pl.semaphore_wait(barrier, len(peers))
    for load in loads:
        load.wait()

    def to_sibling(n, lo, count, recv):
        part = row_pan.at[n, :, pl.ds(lo, count), :]
        return pltpu.make_async_remote_copy(part, part, row_send.at[n, 0], row_recv.at[n, recv],
                                            device_id={'sub': other_sub}, device_id_type=MESH)

    def to_chip(n, lo, count, sub_to):
        part = row_pan.at[n, :, pl.ds(lo, count), :]
        return pltpu.make_async_remote_copy(part, part, row_send.at[n, 1], row_recv.at[n, 0],
                                            device_id={'row': other_x, 'sub': sub_to}, device_id_type=MESH)

    def relay(n, lo):
        part = row_pan.at[n, :, pl.ds(lo, half), :]
        return pltpu.make_async_remote_copy(part, part, relay_send.at[n], row_recv.at[n, 1],
                                            device_id={'sub': other_sub}, device_id_type=MESH)

    def col_copy(n, b):
        part = col_pan.at[n, b]
        return pltpu.make_async_remote_copy(part, part, col_send.at[n], col_recv.at[n, b],
                                            device_id={'col': other_c}, device_id_type=MESH)

    def diag_copy(n):
        return pltpu.make_async_remote_copy(diag.at[n], diag.at[n], diag_send.at[n], diag_recv.at[n],
                                            device_id={'col': other_c}, device_id_type=MESH)

    def out_copies(b):
        return [pltpu.make_async_copy(cur.at[j, block(b, 0, blk)], o_hbm.at[b, :, j * blk:(j + 1) * blk],
                                      out_sem.at[b, j])
                for j in range(col_blks)]

    def one_round(step, carry):
        k = step - 1
        nxt = step
        has_main = step > 0
        has_next = step < rounds
        own_k = (step + row_devs - 1) % row_devs
        own_n = step % row_devs
        is_owner = has_main & (r == own_k)
        is_next = has_next & (r == own_n)
        col_owner = has_main & (c == (step + col_devs - 1) % col_devs)
        col_next = has_next & (c == step % col_devs)
        first = ((step - r + 2 + row_devs) // row_devs + row_blks - 1) % row_blks
        k_c = lax.max(k, 0)
        n_c = lax.min(nxt, rounds - 1)
        q = n_c // col_devs
        far_k = x != own_k // sub_devs
        far_n = has_next & (x != own_n // sub_devs)
        my_lo = sub * half
        other_lo = other_sub * half

        @pl.when(has_main & far_k)
        def _():
            pltpu.make_async_remote_copy(
                row_pan.at[k_c, :, pl.ds(other_lo, half), :], row_pan.at[k_c, :, pl.ds(other_lo, half), :],
                relay_send.at[k_c], row_recv.at[k_c, 1], device_id={'sub': other_sub}, device_id_type=MESH).wait_recv()

        @pl.when(has_main & jnp.logical_not(far_k) & jnp.logical_not(is_owner))
        def _():
            to_sibling(k_c, 0, blk, 0).wait_recv()

        def update(b, lo_chunk, count):
            def one_chunk(h, carry):
                lo = pl.multiple_of((lo_chunk + h) * CHUNK, CHUNK)
                mine = cur.at[:, block(b, lo, CHUNK), :]
                min_plus_rows(col_pan.at[k_c, b, pl.ds(lo, CHUNK), :], row_pan.at[k_c, :, 0:blk, :], mine, mine)
                return carry
            lax.fori_loop(0, count, one_chunk, 0)

        def one_half(t, carry):
            i = t // 2
            h = t % 2
            b = (first + i) % row_blks
            active = has_main & jnp.logical_not(is_owner & (i == 0))

            @pl.when(active & (h == 0) & jnp.logical_not(col_owner))
            def _():
                col_copy(k_c, b).wait_recv()

            update(b, h * (chunks // 2), jnp.where(active, chunks // 2, 0))

            @pl.when((h == 1) & col_next)
            def _():
                col_pan[n_c, b] = cur[q, block(b, 0, blk), :]

                @pl.when(jnp.logical_not(is_next & (i == 0)))
                def _():
                    col_copy(n_c, b).start()

            @pl.when((h == 1) & (step == rounds))
            def _():
                for copy in out_copies(b):
                    copy.start()

            @pl.when((t == 1) & is_next & col_next)
            def _():
                close_block(col_pan.at[n_c, b], diag.at[n_c], spread)
                diag_copy(n_c).start()

            @pl.when(is_next & (t == jnp.where(col_next, 1, PANEL_AT)))
            def _():
                @pl.when(jnp.logical_not(col_next))
                def _():
                    diag_copy(n_c).wait_recv()

                def panel_chunk(h, carry):
                    at = pl.multiple_of(h * PANEL_CHUNK, PANEL_CHUNK)
                    min_plus_rows(diag.at[n_c, pl.ds(at, PANEL_CHUNK), :], cur.at[:, block(first, 0, blk), :],
                                  cur.at[:, block(first, at, PANEL_CHUNK), :],
                                  row_pan.at[n_c, :, pl.ds(at, PANEL_CHUNK), :])
                    to_sibling(n_c, at, PANEL_CHUNK, 0).start()
                    to_chip(n_c, at, PANEL_CHUNK, at // half).start()
                    return carry
                lax.fori_loop(0, blk // PANEL_CHUNK, panel_chunk, 0)
                cur[:, block(first, 0, blk), :] = row_pan[n_c, :, 0:blk, :]

            @pl.when((t == RELAY_AT) & far_n)
            def _():
                to_chip(n_c, my_lo, half, sub).wait_recv()
                relay(n_c, my_lo).start()
            return carry

        lax.fori_loop(0, 2 * row_blks, one_half, 0)

        @pl.when(is_owner)
        def _():
            to_sibling(k_c, 0, blk, 0).wait_send()
            to_chip(k_c, 0, blk, 0).wait_send()

        @pl.when(is_owner & col_owner)
        def _():
            diag_copy(k_c).wait_send()

        @pl.when(has_main & far_k)
        def _():
            relay(k_c, my_lo).wait_send()

        @pl.when(col_owner)
        def _():
            for i in range(row_blks):
                @pl.when(jnp.logical_not(is_owner & (first == i)))
                def _():
                    col_copy(k_c, i).wait_send()
        return carry

    lax.fori_loop(0, rounds + 1, one_round, 0)
    for b in range(row_blks):
        for copy in out_copies(b):
            copy.wait()


def solution(mesh):
    sub_devs = mesh.shape['sub']
    row_devs = mesh.shape['row'] * sub_devs
    col_devs = mesh.shape['col']
    dist_spec = P(('parts', 'row', 'sub'), None, 'col')

    def local_run(local_dist):
        row_blks, blk, cols_width = local_dist.shape
        col_blks = cols_width // blk
        rounds = row_blks * row_devs
        dma = pltpu.SemaphoreType.DMA
        return pl.pallas_call(
            functools.partial(kernel, rounds, row_devs, sub_devs),
            out_shape=jax.ShapeDtypeStruct(local_dist.shape, local_dist.dtype),
            in_specs=[pl.BlockSpec(memory_space=pl.ANY)],
            out_specs=pl.BlockSpec(memory_space=pl.ANY),
            scratch_shapes=[
                pltpu.VMEM((col_blks, row_blks * blk + PAD, blk), jnp.float32),
                pltpu.VMEM((rounds, col_blks, blk + PAD, blk), jnp.float32),
                pltpu.VMEM((rounds, row_blks, blk, blk), jnp.float32),
                pltpu.VMEM((rounds, blk, blk), jnp.float32),
                pltpu.VMEM((GROUP + 1, GROUP, blk), jnp.float32),
                dma((row_blks, col_blks)), dma((row_blks, col_blks)),
                dma((rounds, 2)), dma((rounds, 2)), dma((rounds,)),
                dma((rounds,)), dma((rounds, row_blks)),
                dma((rounds,)), dma((rounds,)),
            ],
            compiler_params=pltpu.CompilerParams(
                collective_id=0, has_side_effects=True, vmem_limit_bytes=40 * 1024 * 1024),
            name='apsp',
        )(local_dist)

    return jax.shard_map(local_run, mesh=mesh, in_specs=(dist_spec,), out_specs=dist_spec, check_vma=False)
```
